32 devices in a mesh: seq: 16 (over z, y, x), head: 2 (over core).
Axes of the slice: x: 2, y: 2, z: 4, core: 2. Of those that a mesh axis runs over, the one named last changes fastest.
Arguments:
- tokens: bfloat16 [16384, 2048], P('seq'), may hold values from -6 to 6
- w_query: bfloat16 [2048, 256], P(None, 'head'), may hold values from -0.25 to 0.25
- w_key: bfloat16 [2048, 256], P(None, 'head'), may hold values from -0.25 to 0.25
- w_value: bfloat16 [2048, 2048], P(None, 'head'), may hold values from -0.125 to 0.125
- w_out: bfloat16 [2048, 2048], replicated, may hold values from -1.796875 to 1.796875
Outputs:
- mixed: bfloat16 [16384, 2048], P('seq', 'head')
The draws below stay inside these ranges and needn't reach their ends.
All inputs are finite; a program needn't handle non-finite values.
Results may differ from the reference program's by a relative error of at most 0.011.
Values may be sent and summed in bfloat16 or wider, within the bound.
A program may use at most 128 MiB of HBM per device.

```python
import jax
import jax.numpy as jnp
from jax import lax

D = 2048
HEADS = 16
KEY_DIM = 16
VALUE_DIM = 128
TOK_DEV = 1024
FEATURES = 273
TOKENS = 16384
N_SEQ = 16


def steps_of(stream_key, extent, split, least, largest):
    factor_of, own = 1.0, jax.random.fold_in(stream_key, 6)
    for axis_at, shards_of in split:
        draws = jnp.exp(jax.random.uniform(jax.random.fold_in(own, axis_at), (shards_of,), jnp.float32, least / len(split), largest / len(split)))
        factor_of = factor_of * jnp.repeat(draws, extent[axis_at] // shards_of).reshape([-1 if axis == axis_at else 1 for axis in range(len(extent))])
    return factor_of


def normal_values(own_key, dims, spread, most, split=(), held_as=jnp.bfloat16):
    result = spread * jax.random.normal(own_key, dims, jnp.float32)
    if split:
        result = result * steps_of(own_key, dims, split, -0.22, 0.18)
    return jnp.clip(result, -most, most).astype(held_as)


def setup_inputs(seed: int = 0) -> dict:
    seeds = jax.random.split(jax.random.key(seed), 6)
    tokens = normal_values(seeds[0], (TOKENS, D), 1.0, 6.0, ((0, 16),))
    w_query = normal_values(seeds[1], (D, HEADS * KEY_DIM), (D // 4) ** -0.5, 0.25, ((1, 2),))
    w_key = normal_values(seeds[2], (D, HEADS * KEY_DIM), (D // 4) ** -0.5, 0.25, ((1, 2),))
    w_value = normal_values(seeds[3], (D, HEADS * VALUE_DIM), D ** -0.5, 0.125, ((1, 2),))
    w_out = normal_values(seeds[4], (HEADS * VALUE_DIM, D), 0.3, 1.796875)
    return dict(tokens=tokens, w_query=w_query, w_key=w_key, w_value=w_value, w_out=w_out)


def taylor_features(rows):
    wide = rows.astype(jnp.float32)
    count = wide.shape[-1]
    outer = (wide[..., :, None] * wide[..., None, :]).reshape(wide.shape[:-1] + (count * count,))
    ones = jnp.ones(wide.shape[:-1] + (1,), jnp.float32)
    joined = jnp.concatenate([ones, wide / (count ** 0.25), outer / ((2.0 * count) ** 0.5)], axis=-1)
    return joined.astype(jnp.bfloat16)


def reference(tokens, w_query, w_key, w_value, w_out):
    def span_step(carry, span_rows):
        prefix, zprefix = carry
        queries = jnp.dot(span_rows, w_query, preferred_element_type=jnp.float32).astype(jnp.bfloat16).reshape(TOK_DEV, HEADS, KEY_DIM)
        key_rows = jnp.dot(span_rows, w_key, preferred_element_type=jnp.float32).astype(jnp.bfloat16).reshape(TOK_DEV, HEADS, KEY_DIM)
        val_rows = jnp.dot(span_rows, w_value, preferred_element_type=jnp.float32).astype(jnp.bfloat16).reshape(TOK_DEV, HEADS, VALUE_DIM)
        query_feat = taylor_features(queries)
        key_feat = taylor_features(key_rows)
        state = jnp.einsum('thf,thv->hfv', key_feat.astype(jnp.float32), val_rows.astype(jnp.float32), precision=lax.Precision.HIGHEST)
        norm_sum = jnp.sum(key_feat.astype(jnp.float32), axis=0)
        prefix_low = prefix.astype(jnp.bfloat16)
        numer_pre = jnp.einsum('thf,hfv->thv', query_feat.astype(jnp.float32), prefix_low.astype(jnp.float32), precision=lax.Precision.HIGHEST)
        denom_pre = jnp.einsum('thf,hf->th', query_feat.astype(jnp.float32), zprefix, precision=lax.Precision.HIGHEST)
        block = min(512, TOK_DEV)
        outputs = []
        for index in range(TOK_DEV // block):
            low = index * block
            high = low + block
            q_block = queries[low:high].astype(jnp.float32)
            k_block = key_rows[:high].astype(jnp.float32)
            scores = jnp.einsum('qhd,khd->hqk', q_block, k_block) / (KEY_DIM ** 0.5)
            taylor = 1.0 + scores + 0.5 * scores * scores
            row_ids = low + jnp.arange(block, dtype=jnp.int32)[:, None]
            col_ids = jnp.arange(high, dtype=jnp.int32)[None, :]
            taylor = jnp.where((col_ids <= row_ids)[None], taylor, 0.0)
            denom = denom_pre[low:high] + jnp.transpose(jnp.sum(taylor, axis=-1))
            taylor_low = taylor.astype(jnp.bfloat16)
            numer_in = jnp.einsum('hqk,khv->qhv', taylor_low.astype(jnp.float32), val_rows[:high].astype(jnp.float32))
            numer = numer_pre[low:high] + numer_in
            outputs.append((numer / denom[..., None]).astype(jnp.bfloat16))
        attended = jnp.concatenate(outputs, axis=0).reshape(TOK_DEV, HEADS * VALUE_DIM)
        mixed_rows = jnp.dot(attended, w_out, preferred_element_type=jnp.float32).astype(jnp.bfloat16)
        return (prefix + state, zprefix + norm_sum), mixed_rows

    init = (jnp.zeros((HEADS, FEATURES, VALUE_DIM), jnp.float32), jnp.zeros((HEADS, FEATURES), jnp.float32))
    spans = tokens.reshape(N_SEQ, TOK_DEV, D)
    final, mixed = lax.scan(span_step, init, spans)
    return mixed.reshape(TOKENS, D)
```

```python
import functools

import jax
import jax.numpy as jnp
from jax import lax
from jax.experimental import pallas as pl
from jax.experimental.pallas import tpu as pltpu
from jax.sharding import PartitionSpec as P

KEY_DIM = 16
VALUE_DIM = 128
ROWS = 160
PAIR = 2
LOADS = 2
PLANE = 4
VMEM_LIMIT = 50 * 1024 * 1024
PIECE = PAIR * ROWS // PLANE
MESH = pl.DeviceIdType.MESH
F32 = jnp.float32
BF16 = jnp.bfloat16


def features(u, tail_one, square):
    n = u.shape[1]
    twice = jnp.concatenate([u, u], axis=0)
    parts = [u, u * u * square]
    for d in range(1, KEY_DIM // 2):
        parts.append(u * twice[d : d + KEY_DIM])
    half = KEY_DIM // 2
    parts.append(u[:half] * u[half:])
    row = lax.broadcasted_iota(jnp.int32, (8, n), 0)
    parts.append(jnp.where(row == 0, tail_one, 0.0))
    return jnp.concatenate(parts, axis=0)


def pack_norm(total):
    state, norm = total[:, :VALUE_DIM], total[:, VALUE_DIM:]
    top = norm[:VALUE_DIM]
    rest = norm[VALUE_DIM:]

    def diagonal(block):
        r = lax.broadcasted_iota(jnp.int32, block.shape, 0)
        l = lax.broadcasted_iota(jnp.int32, block.shape, 1)
        return jnp.sum(jnp.where(r == l, block, 0.0), axis=0, keepdims=True)

    first, second = diagonal(top), diagonal(rest)
    r = lax.broadcasted_iota(jnp.int32, (8, VALUE_DIM), 0)
    tail = jnp.where(r == 0, state[ROWS - 8 :], jnp.where(r == 1, first, jnp.where(r == 2, second, 0.0)))
    return jnp.concatenate([state[: ROWS - 8], tail], axis=0)


def unpack_norm(packed):
    tail = packed[ROWS - 8 :]

    def column(row, height):
        r = lax.broadcasted_iota(jnp.int32, (height, VALUE_DIM), 0)
        l = lax.broadcasted_iota(jnp.int32, (height, VALUE_DIM), 1)
        return jnp.sum(jnp.where(r == l, row, 0.0), axis=1, keepdims=True)

    return jnp.concatenate([column(tail[1:2], VALUE_DIM), column(tail[2:3], ROWS - VALUE_DIM)], axis=0)


def kernel(
    n_seq, chunk,
    tok_hbm, wq_hbm, wk_hbm, wv_hbm, wo_hbm, out_ref,
    tok, wqk, wv, wo, vals, qs, qt, kt, kfeat, local, inner, qfeat,
    send_s, recv_s, send_z, recv_z, send_b, recv_b,
    acc, load_sem, tok_sem, v_sem, o_sem, s_ss, s_rs, z_ss, z_rs, b_ss, b_rs, a_ss, a_rs, free_sem,
):
    att = tok
    blocks, rows, block = tok.shape
    heads = vals.shape[0]
    groups = heads // PAIR
    chunks = rows // chunk
    out_blocks = wo.shape[0]
    cols_here = out_blocks * block
    planes = n_seq // PLANE
    seq = lax.axis_index("seq")
    core = lax.axis_index("head")
    p = lax.rem(seq, PLANE)
    z = seq // PLANE
    first = z * PLANE
    peers = [lax.rem(p + o, PLANE) for o in range(1, PLANE)]

    part_rows = rows // LOADS
    load_w = [
        pltpu.make_async_copy(wk_hbm, wqk.at[:, pl.ds(128, 128)], load_sem.at[1]),
        pltpu.make_async_copy(wq_hbm, wqk.at[:, pl.ds(0, 128)], load_sem.at[0]),
    ]
    load_t = [
        [
            pltpu.make_async_copy(
                tok_hbm.at[pl.ds(i * part_rows, part_rows), pl.ds(b * block, block)],
                tok.at[b, pl.ds(i * part_rows, part_rows)], tok_sem.at[i, b])
            for b in range(blocks)
        ]
        for i in range(LOADS)
    ]
    load_o = [
        pltpu.make_async_copy(
            wo_hbm.at[:, pl.ds(pl.multiple_of(core * cols_here + b * block, 128), block)], wo.at[b], o_sem.at[b])
        for b in range(out_blocks)
    ]
    step = PAIR * VALUE_DIM

    def load_v(g):
        return pltpu.make_async_copy(wv_hbm.at[:, pl.ds(g * step, step)], wv.at[g], v_sem.at[g])

    for c in load_w:
        c.start()
    for i in range(LOADS):
        for c in load_t[i]:
            c.start(priority=min(i, 1))

    barrier = pltpu.get_barrier_semaphore()
    for q in peers:
        pl.semaphore_signal(barrier, inc=1, device_id=(first + q, core), device_id_type=MESH)
    for o in range(1, planes):
        there = lax.rem(z + o, planes) * PLANE + p
        pl.semaphore_signal(barrier, inc=1, device_id=(there, core), device_id_type=MESH)
    pl.semaphore_signal(barrier, inc=1, device_id=(seq, 1 - core), device_id_type=MESH)
    greetings = PLANE - 1 + planes - 1 + 1

    def copy_s(g, q, slot):
        return pltpu.make_async_remote_copy(
            src_ref=send_s.at[g, q], dst_ref=recv_s.at[g, slot], send_sem=s_ss.at[g, q], recv_sem=s_rs.at[g, slot],
            device_id=(first + q, core), device_id_type=MESH)

    def copy_z(g, there, slot):
        return pltpu.make_async_remote_copy(
            src_ref=send_z.at[g], dst_ref=recv_z.at[g, slot], send_sem=z_ss.at[g, there], recv_sem=z_rs.at[g, slot],
            device_id=(there * PLANE + p, core), device_id_type=MESH)

    def copy_b(g, q, slot):
        return pltpu.make_async_remote_copy(
            src_ref=send_b.at[g, q], dst_ref=recv_b.at[g, slot], send_sem=b_ss.at[g, q], recv_sem=b_rs.at[g, slot],
            device_id=(first + q, core), device_id_type=MESH)

    own_at, peer_at = core * groups, (1 - core) * groups

    def copy_a(g, base):
        return pltpu.make_async_remote_copy(
            src_ref=att.at[base + g], dst_ref=att.at[base + g], send_sem=a_ss.at[g], recv_sem=a_rs.at[g],
            device_id=(seq, 1 - core), device_id_type=MESH)

    def gather_pieces(g):
        for q in peers:
            copy_s(g, q, p).start()

    def send_up(g):
        for q in peers:
            copy_s(g, q, q).wait_recv()
        total = recv_s[g, 0].astype(F32)
        for q in range(1, PLANE):
            total = total + recv_s[g, q].astype(F32)
        send_z[g] = total.astype(BF16)

        def send(i, _):
            copy_z(g, planes - 1 - i, z).start()
            return 0

        lax.fori_loop(0, planes - 1 - z, send, 0)

    def give_back(g):
        def take(i, total):
            copy_z(g, i, i).wait_recv()
            return total + recv_z[g, i].astype(F32)

        total = lax.fori_loop(0, z, take, jnp.zeros((PIECE, VALUE_DIM), F32))
        for q in range(PLANE):
            send_b[g, q] = total.astype(BF16)
            total = total + recv_s[g, q].astype(F32)
        for q in peers:
            copy_b(g, q, p).start()
        recv_b[g, p] = send_b[g, p]

    def token_rows(begin, end):
        return jnp.concatenate([tok[b, pl.ds(begin, end - begin)] for b in range(blocks)], axis=1)

    for c in load_w:
        c.wait()
    for i in range(LOADS):
        for c in load_t[i]:
            c.wait()
        if i == 0:
            for g in range(groups):
                load_v(g).start(priority=1)
        part = pl.ds(i * part_rows, part_rows)
        qk = jnp.dot(token_rows(i * part_rows, (i + 1) * part_rows), wqk[...], preferred_element_type=F32)
        qk = qk.astype(BF16).astype(F32)
        q = qk[:, :128] * 0.25
        qs[part] = q.astype(BF16)
        for c in range(part_rows // chunk):
            at = i * (part_rows // chunk) + c
            qt[at] = q[c * chunk : (c + 1) * chunk].T
            kt[at] = qk[c * chunk : (c + 1) * chunk, 128:].T
    for c in load_o:
        c.start(priority=1)

    def head_rows(h):
        if isinstance(h, int):
            return pl.ds(h * KEY_DIM, KEY_DIM)
        return pl.ds(pl.multiple_of(h * KEY_DIM, KEY_DIM), KEY_DIM)

    def key_features(g):
        for i in range(PAIR):
            h = g * PAIR + i
            for c in range(chunks):
                kfeat[h % (2 * PAIR), c] = features(kt[c, head_rows(h)], 1.0, 1.0).astype(BF16)

    def values(g, begin, end):
        part = pl.ds(begin, end - begin)
        v = jnp.dot(token_rows(begin, end), wv[g], preferred_element_type=F32).astype(BF16)
        for i in range(PAIR):
            vals[g * PAIR + i, part] = v[:, i * VALUE_DIM : (i + 1) * VALUE_DIM]

    def states(g):
        ones = jnp.ones((chunk, VALUE_DIM), BF16)
        for i in range(PAIR):
            h = g * PAIR + i
            total = jnp.zeros((ROWS, 2 * VALUE_DIM), F32)
            for c in range(chunks):
                span = pl.ds(c * chunk, chunk)
                local[h, c] = total
                wide = jnp.concatenate([vals[h, span], ones], axis=1)
                total = total + jnp.dot(kfeat[h % (2 * PAIR), c], wide, preferred_element_type=F32)
            packed = pack_norm(total).astype(BF16)
            send_s[g, 2 * i] = packed[:PIECE]
            send_s[g, 2 * i + 1] = packed[PIECE:]
        recv_s[g, p] = send_s[g, p]

    for g in range(groups):
        load_v(g).wait()
        values(g, 0, rows // 2)
        key_features(g)
        if g > 0:
            states(g - 1)
        values(g, rows // 2, rows)
        if g > 0:
            if g == 1:
                pl.semaphore_wait(barrier, greetings)
            gather_pieces(g - 1)
    pl.semaphore_signal(free_sem, inc=1, device_id=(seq, 1 - core), device_id_type=MESH)
    states(groups - 1)
    gather_pieces(groups - 1)

    def inner_head(h):
        row_head = lax.broadcasted_iota(jnp.int32, (128, chunk), 0) // KEY_DIM
        r = lax.broadcasted_iota(jnp.int32, (chunk, chunk), 0)
        l = lax.broadcasted_iota(jnp.int32, (chunk, chunk), 1)
        ones = jnp.ones((chunk, VALUE_DIM), BF16)
        for c in range(chunks):
            span = pl.ds(c * chunk, chunk)
            k_own = jnp.where(row_head == h, kt[c], 0.0).astype(BF16)
            s = jnp.dot(qs[span], k_own, preferred_element_type=F32)
            s1 = s + 1.0
            taylor = jnp.where(l <= r, 0.5 * (s1 * s1) + 0.5, 0.0).astype(BF16)
            wide = jnp.concatenate([vals[h, span], ones], axis=1)
            inner[h, span] = jnp.dot(taylor, wide, preferred_element_type=F32)
            feat = features(qt[c, head_rows(h)], 1.0, 0.5)
            qfeat[h, span] = feat.T.astype(BF16)

    def inner_step(g, _):
        for i in range(PAIR):
            inner_head(g * PAIR + i)
        send_up(g)
        return 0

    lax.fori_loop(0, groups, inner_step, 0)

    def back_step(g, _):
        give_back(g)
        return 0

    lax.fori_loop(0, groups, back_step, 0)

    def outer(g):
        for q in peers:
            copy_b(g, q, q).wait_recv()
        for i in range(PAIR):
            h = g * PAIR + i
            packed = jnp.concatenate([recv_b[g, 2 * i], recv_b[g, 2 * i + 1]], axis=0).astype(F32)
            norm = jnp.broadcast_to(unpack_norm(packed), (ROWS, VALUE_DIM))
            entering = jnp.concatenate([packed, norm], axis=1)
            for c in range(chunks):
                span = pl.ds(c * chunk, chunk)
                prefix = (entering + local[h, c]).astype(BF16)
                total = inner[h, span] + jnp.dot(qfeat[h, span], prefix, preferred_element_type=F32)
                result = total[:, :VALUE_DIM] / total[:, VALUE_DIM:]
                att[own_at + g, span, pl.ds(i * VALUE_DIM, VALUE_DIM)] = result.astype(BF16)
        copy_a(g, own_at).start()

    def project(g, begin, end):
        copy_a(g, peer_at).wait_recv()
        here = pl.ds(pl.multiple_of((own_at + g) * step, step), step)
        there = pl.ds(pl.multiple_of((peer_at + g) * step, step), step)
        both = jnp.concatenate([att[own_at + g], att[peer_at + g]], axis=1)
        for b in range(out_blocks):
            w = jnp.concatenate([wo[b, here], wo[b, there]], axis=0)
            part = jnp.dot(both, w, preferred_element_type=F32)
            if not begin:
                part = part + acc[b]
            if end:
                out_ref[:, pl.ds(b * block, block)] = part.astype(BF16)
            else:
                acc[b] = part

    pl.semaphore_wait(free_sem, 1)
    outer(0)
    for c in load_o:
        c.wait()
    for g in range(1, groups):
        outer(g)
        project(g - 1, g == 1, False)
    project(groups - 1, False, True)

    def finish(g, _):
        copy_a(g, own_at).wait_send()
        for q in peers:
            copy_s(g, q, p).wait_send()
            copy_b(g, q, p).wait_send()

        def sent(i, _):
            copy_z(g, planes - 1 - i, z).wait_send()
            return 0

        lax.fori_loop(0, planes - 1 - z, sent, 0)
        return 0

    lax.fori_loop(0, groups, finish, 0)


def per_device(tokens, w_query, w_key, w_value, w_out):
    n_seq = lax.axis_size("seq")
    rows, width = tokens.shape
    heads = w_query.shape[1] // KEY_DIM
    groups = heads // PAIR
    planes = n_seq // PLANE
    chunk = min(256, rows)
    block = PAIR * VALUE_DIM
    cols = w_out.shape[1] // lax.axis_size("head")
    vm = pltpu.VMEM
    dma = pltpu.SemaphoreType.DMA
    return pl.pallas_call(
        functools.partial(kernel, n_seq, chunk),
        out_shape=jax.ShapeDtypeStruct((rows, cols), BF16),
        in_specs=[pl.BlockSpec(memory_space=pltpu.HBM)] * 5,
        out_specs=pl.BlockSpec(memory_space=pltpu.VMEM),
        scratch_shapes=[
            vm((width // block, rows, block), BF16),
            vm((width, 256), BF16),
            vm((groups, width, PAIR * VALUE_DIM), BF16),
            vm((cols // block, w_out.shape[0], block), BF16),
            vm((heads, rows, VALUE_DIM), BF16),
            vm((rows, 128), BF16),
            vm((rows // chunk, 128, chunk), F32),
            vm((rows // chunk, 128, chunk), F32),
            vm((2 * PAIR, rows // chunk, ROWS, chunk), BF16),
            vm((heads, rows // chunk, ROWS, 2 * VALUE_DIM), F32),
            vm((heads, rows, 2 * VALUE_DIM), F32),
            vm((heads, rows, ROWS), BF16),
            vm((groups, PLANE, PIECE, VALUE_DIM), BF16),
            vm((groups, PLANE, PIECE, VALUE_DIM), BF16),
            vm((groups, PIECE, VALUE_DIM), BF16),
            vm((groups, planes, PIECE, VALUE_DIM), BF16),
            vm((groups, PLANE, PIECE, VALUE_DIM), BF16),
            vm((groups, PLANE, PIECE, VALUE_DIM), BF16),
            vm((cols // block, rows, block), F32),
            dma((2,)), dma((LOADS, width // block)), dma((groups,)), dma((cols // block,)),
            dma((groups, PLANE)), dma((groups, PLANE)),
            dma((groups, planes)), dma((groups, planes)),
            dma((groups, PLANE)), dma((groups, PLANE)),
            dma((groups,)), dma((groups,)), pltpu.SemaphoreType.REGULAR,
        ],
        compiler_params=pltpu.CompilerParams(
            collective_id=0, has_side_effects=True, vmem_limit_bytes=VMEM_LIMIT
        ),
    )(*(pltpu.with_memory_space_constraint(a, pltpu.HBM) for a in (tokens, w_query, w_key, w_value, w_out)))


def solution(mesh):
    in_specs = (P("seq", None), P(None, "head"), P(None, "head"), P(None, "head"), P())
    return jax.shard_map(
        per_device, mesh=mesh, in_specs=in_specs, out_specs=P("seq", "head"), check_vma=False
    )
```

```python
import functools

import jax
import jax.numpy as jnp
from jax import lax
from jax.experimental import pallas as pl
from jax.experimental.pallas import tpu as pltpu
from jax.sharding import PartitionSpec as P

KEY_DIM = 16
VALUE_DIM = 128
ROWS = 160
PAIR = 2
LOADS = 2
PLANE = 4
VMEM_LIMIT = 51 * 1024 * 1024
PIECE = PAIR * ROWS // PLANE
MESH = pl.DeviceIdType.MESH
F32 = jnp.float32
BF16 = jnp.bfloat16


def features(u, tail_one, square):
    n = u.shape[1]
    twice = jnp.concatenate([u, u], axis=0)
    parts = [u, u * u * square]
    for d in range(1, KEY_DIM // 2):
        parts.append(u * twice[d : d + KEY_DIM])
    half = KEY_DIM // 2
    parts.append(u[:half] * u[half:])
    row = lax.broadcasted_iota(jnp.int32, (8, n), 0)
    parts.append(jnp.where(row == 0, tail_one, 0.0))
    return jnp.concatenate(parts, axis=0)


def pack_norm(total):
    state, norm = total[:, :VALUE_DIM], total[:, VALUE_DIM:]
    top = norm[:VALUE_DIM]
    rest = norm[VALUE_DIM:]

    def diagonal(block):
        r = lax.broadcasted_iota(jnp.int32, block.shape, 0)
        l = lax.broadcasted_iota(jnp.int32, block.shape, 1)
        return jnp.sum(jnp.where(r == l, block, 0.0), axis=0, keepdims=True)

    first, second = diagonal(top), diagonal(rest)
    r = lax.broadcasted_iota(jnp.int32, (8, VALUE_DIM), 0)
    tail = jnp.where(r == 0, state[ROWS - 8 :], jnp.where(r == 1, first, jnp.where(r == 2, second, 0.0)))
    return jnp.concatenate([state[: ROWS - 8], tail], axis=0)


def unpack_norm(packed):
    tail = packed[ROWS - 8 :]

    def column(row, height):
        r = lax.broadcasted_iota(jnp.int32, (height, VALUE_DIM), 0)
        l = lax.broadcasted_iota(jnp.int32, (height, VALUE_DIM), 1)
        return jnp.sum(jnp.where(r == l, row, 0.0), axis=1, keepdims=True)

    return jnp.concatenate([column(tail[1:2], VALUE_DIM), column(tail[2:3], ROWS - VALUE_DIM)], axis=0)


def kernel(
    n_seq, chunk,
    tok_hbm, wq_hbm, wk_hbm, wv_hbm, wo_hbm, out_ref,
    tok, wqkv, wo, vals, qs, qt, kt, kfeat, local, inner, qfeat,
    send_s, recv_s, send_z, recv_z, send_b, recv_b,
    acc, w_sem, tok_sem, o_sem, s_ss, s_rs, z_ss, z_rs, b_ss, b_rs, a_ss, a_rs, free_sem,
):
    att = tok
    blocks, rows, block = tok.shape
    heads = vals.shape[0]
    groups = heads // PAIR
    chunks = rows // chunk
    out_blocks = wo.shape[0]
    cols_here = out_blocks * block
    planes = n_seq // PLANE
    seq = lax.axis_index("seq")
    core = lax.axis_index("head")
    p = lax.rem(seq, PLANE)
    z = seq // PLANE
    first = z * PLANE
    peers = [PLANE - 1 - p, p + 1 - 2 * lax.rem(p, 2), lax.rem(p + 2, PLANE)]

    part_rows = rows // LOADS
    left, right = pl.ds(0, VALUE_DIM), pl.ds(VALUE_DIM, VALUE_DIM)
    load_w = [[
        pltpu.make_async_copy(wk_hbm, wqkv.at[0, :, left], w_sem.at[0, 0]),
        pltpu.make_async_copy(wv_hbm.at[:, left], wqkv.at[0, :, right], w_sem.at[0, 1]),
    ]]
    for x in range(1, groups):
        at = pl.ds((2 * x - 1) * VALUE_DIM, block)
        load_w.append([pltpu.make_async_copy(wv_hbm.at[:, at], wqkv.at[x], w_sem.at[x, 0])])
    at = pl.ds((heads - 1) * VALUE_DIM, VALUE_DIM)
    load_w.append([
        pltpu.make_async_copy(wv_hbm.at[:, at], wqkv.at[groups, :, left], w_sem.at[groups, 0]),
        pltpu.make_async_copy(wq_hbm, wqkv.at[groups, :, right], w_sem.at[groups, 1]),
    ])
    load_t = [
        [
            pltpu.make_async_copy(
                tok_hbm.at[pl.ds(i * part_rows, part_rows), pl.ds(b * block, block)],
                tok.at[b, pl.ds(i * part_rows, part_rows)], tok_sem.at[i, b])
            for b in range(blocks)
        ]
        for i in range(LOADS)
    ]
    load_o = [
        pltpu.make_async_copy(
            wo_hbm.at[:, pl.ds(pl.multiple_of(core * cols_here + b * block, 128), block)], wo.at[b], o_sem.at[b])
        for b in range(out_blocks)
    ]
    step = PAIR * VALUE_DIM

    for c in load_w[0]:
        c.start()
    for i in range(LOADS):
        for c in load_t[i]:
            c.start()
    for x in range(1, groups + 1):
        for c in load_w[x]:
            c.start(priority=1)

    barrier = pltpu.get_barrier_semaphore()
    for q in peers:
        pl.semaphore_signal(barrier, inc=1, device_id=(first + q, core), device_id_type=MESH)
    for o in range(1, planes):
        there = lax.rem(z + o, planes) * PLANE + p
        pl.semaphore_signal(barrier, inc=1, device_id=(there, core), device_id_type=MESH)
    pl.semaphore_signal(barrier, inc=1, device_id=(seq, 1 - core), device_id_type=MESH)
    greetings = PLANE - 1 + planes - 1 + 1

    def copy_s(g, q, slot):
        return pltpu.make_async_remote_copy(
            src_ref=send_s.at[g, q], dst_ref=recv_s.at[g, slot], send_sem=s_ss.at[g, q], recv_sem=s_rs.at[g, slot],
            device_id=(first + q, core), device_id_type=MESH)

    def copy_z(g, there, slot):
        return pltpu.make_async_remote_copy(
            src_ref=send_z.at[g], dst_ref=recv_z.at[g, slot], send_sem=z_ss.at[g, there], recv_sem=z_rs.at[g, slot],
            device_id=(there * PLANE + p, core), device_id_type=MESH)

    def copy_b(g, q, slot):
        return pltpu.make_async_remote_copy(
            src_ref=send_b.at[g, q], dst_ref=recv_b.at[g, slot], send_sem=b_ss.at[g, q], recv_sem=b_rs.at[g, slot],
            device_id=(first + q, core), device_id_type=MESH)

    own_at, peer_at = core * groups, (1 - core) * groups

    def copy_a(g, base):
        return pltpu.make_async_remote_copy(
            src_ref=att.at[base + g], dst_ref=att.at[base + g], send_sem=a_ss.at[g], recv_sem=a_rs.at[g],
            device_id=(seq, 1 - core), device_id_type=MESH)

    def gather_pieces(g):
        recv_s[g, p] = send_s[g, p]
        for q in peers:
            copy_s(g, q, p).start()

    def send_up(g):
        for q in peers:
            copy_s(g, q, q).wait_recv()
        total = recv_s[g, 0].astype(F32)
        for q in range(1, PLANE):
            total = total + recv_s[g, q].astype(F32)
        send_z[g] = total.astype(BF16)

        def send(i, _):
            copy_z(g, i if g % 2 else planes + z - i, z).start()
            return 0

        lax.fori_loop(z + 1, planes, send, 0)

    def give_back(g):
        def take(i, total):
            copy_z(g, i, i).wait_recv()
            return total + recv_z[g, i].astype(F32)

        total = lax.fori_loop(0, z, take, jnp.zeros((PIECE, VALUE_DIM), F32))
        for q in range(PLANE):
            send_b[g, q] = total.astype(BF16)
            total = total + recv_s[g, q].astype(F32)
        for q in peers:
            copy_b(g, q, p).start()
        recv_b[g, p] = send_b[g, p]

    def token_rows(begin, end):
        return jnp.concatenate([tok[b, pl.ds(begin, end - begin)] for b in range(blocks)], axis=1)

    def head_rows(h):
        if isinstance(h, int):
            return pl.ds(h * KEY_DIM, KEY_DIM)
        return pl.ds(pl.multiple_of(h * KEY_DIM, KEY_DIM), KEY_DIM)

    def transposed(ref, part, begin):
        for c in range(part.shape[0] // chunk):
            ref[begin // chunk + c] = part[c * chunk : (c + 1) * chunk].T

    def project_in(x, begin, end):
        part = pl.ds(begin, end - begin)
        tokens = jnp.concatenate([tok[b, part] for b in range(blocks)], axis=1)
        both = jnp.dot(tokens, wqkv[x], preferred_element_type=F32).astype(BF16)
        lo, hi = both[:, :VALUE_DIM], both[:, VALUE_DIM:]
        if x == 0:
            transposed(kt, lo.astype(F32), begin)
            vals[0, part] = hi
            return
        vals[2 * x - 1, part] = lo
        if x < groups:
            vals[2 * x, part] = hi
            return
        q = hi.astype(F32) * 0.25
        qs[part] = q.astype(BF16)
        transposed(qt, q, begin)

    def key_features(h):
        for c in range(chunks):
            kfeat[h, c] = features(kt[c, head_rows(h)], 1.0, 1.0).astype(BF16)

    def state(h):
        ones = jnp.ones((chunk, VALUE_DIM), BF16)
        total = jnp.zeros((ROWS, 2 * VALUE_DIM), F32)
        for c in range(chunks):
            span = pl.ds(c * chunk, chunk)
            local[h, c] = total
            wide = jnp.concatenate([vals[h, span], ones], axis=1)
            total = total + jnp.dot(kfeat[h, c], wide, preferred_element_type=F32)
        packed = pack_norm(total).astype(BF16)
        g, i = h // PAIR, h % PAIR
        send_s[g, 2 * i] = packed[:PIECE]
        send_s[g, 2 * i + 1] = packed[PIECE:]

    for c in load_w[0]:
        c.wait()
    for i in range(LOADS):
        for c in load_t[i]:
            c.wait()
        project_in(0, i * part_rows, (i + 1) * part_rows)
    for c in load_o:
        c.start(priority=1)

    for x in range(1, groups + 1):
        for c in load_w[x]:
            c.wait()
        if x == 1:
            key_features(0)
        key_features(2 * x - 1)
        project_in(x, 0, rows // 2)
        if x > 2:
            state(2 * x - 3)
        state(2 * x - 2)
        if x < groups:
            key_features(2 * x)
        project_in(x, rows // 2, rows)
        if x == 1:
            pl.semaphore_wait(barrier, greetings)
            state(1)
            gather_pieces(0)
        if x > 2:
            gather_pieces(x - 2)
    pl.semaphore_signal(free_sem, inc=1, device_id=(seq, 1 - core), device_id_type=MESH)
    state(heads - 1)
    gather_pieces(groups - 1)

    def inner_head(h):
        row_head = lax.broadcasted_iota(jnp.int32, (128, chunk), 0) // KEY_DIM
        r = lax.broadcasted_iota(jnp.int32, (chunk, chunk), 0)
        l = lax.broadcasted_iota(jnp.int32, (chunk, chunk), 1)
        ones = jnp.ones((chunk, VALUE_DIM), BF16)
        for c in range(chunks):
            span = pl.ds(c * chunk, chunk)
            k_own = jnp.where(row_head == h, kt[c], 0.0).astype(BF16)
            s = jnp.dot(qs[span], k_own, preferred_element_type=F32)
            s1 = s + 1.0
            taylor = jnp.where(l <= r, 0.5 * (s1 * s1) + 0.5, 0.0).astype(BF16)
            wide = jnp.concatenate([vals[h, span], ones], axis=1)
            inner[h, span] = jnp.dot(taylor, wide, preferred_element_type=F32)
            feat = features(qt[c, head_rows(h)], 1.0, 0.5)
            qfeat[h, span] = feat.T.astype(BF16)

    def outer(g):
        for q in peers:
            copy_b(g, q, q).wait_recv()
        for i in range(PAIR):
            h = g * PAIR + i
            packed = jnp.concatenate([recv_b[g, 2 * i], recv_b[g, 2 * i + 1]], axis=0).astype(F32)
            norm = jnp.broadcast_to(unpack_norm(packed), (ROWS, VALUE_DIM))
            entering = jnp.concatenate([packed, norm], axis=1)
            for c in range(chunks):
                span = pl.ds(c * chunk, chunk)
                prefix = (entering + local[h, c]).astype(BF16)
                total = inner[h, span] + jnp.dot(qfeat[h, span], prefix, preferred_element_type=F32)
                result = total[:, :VALUE_DIM] / total[:, VALUE_DIM:]
                att[own_at + g, span, pl.ds(i * VALUE_DIM, VALUE_DIM)] = result.astype(BF16)
        copy_a(g, own_at).start()

    def project(g, own, peer, begin, end):
        bases = ([own_at] if own else []) + ([peer_at] if peer else [])
        if peer:
            copy_a(g, peer_at).wait_recv()
        rows_of = [pl.ds(pl.multiple_of((base + g) * step, step), step) for base in bases]
        both = jnp.concatenate([att[base + g] for base in bases], axis=1)
        for b in range(out_blocks):
            w = jnp.concatenate([wo[b, r] for r in rows_of], axis=0)
            part = jnp.dot(both, w, preferred_element_type=F32)
            if not begin:
                part = part + acc[b]
            if end:
                out_ref[:, pl.ds(b * block, block)] = part.astype(BF16)
            else:
                acc[b] = part

    def inner_pair(g):
        for i in range(PAIR):
            inner_head(g * PAIR + i)

    last = groups - 1
    send_up(0)
    inner_pair(0)
    for g in range(1, last):
        inner_pair(g)
        send_up(g)
    send_up(last)
    give_back(0)
    inner_pair(last)
    for g in range(1, last):
        give_back(g)
    pl.semaphore_wait(free_sem, 1)
    outer(0)
    give_back(last)
    for c in load_o:
        c.wait()
    for g in range(1, groups):
        outer(g)
        project(g - 1, True, True, g == 1, False)
    project(last, True, False, False, False)
    project(last, False, True, False, True)

    def finish(g, _):
        copy_a(g, own_at).wait_send()
        for q in peers:
            copy_s(g, q, p).wait_send()
            copy_b(g, q, p).wait_send()

        def sent(i, _):
            copy_z(g, planes - 1 - i, z).wait_send()
            return 0

        lax.fori_loop(0, planes - 1 - z, sent, 0)
        return 0

    lax.fori_loop(0, groups, finish, 0)


def per_device(tokens, w_query, w_key, w_value, w_out):
    n_seq = lax.axis_size("seq")
    rows, width = tokens.shape
    heads = w_query.shape[1] // KEY_DIM
    groups = heads // PAIR
    planes = n_seq // PLANE
    chunk = min(256, rows)
    block = PAIR * VALUE_DIM
    cols = w_out.shape[1] // lax.axis_size("head")
    vm = pltpu.VMEM
    dma = pltpu.SemaphoreType.DMA
    return pl.pallas_call(
        functools.partial(kernel, n_seq, chunk),
        out_shape=jax.ShapeDtypeStruct((rows, cols), BF16),
        in_specs=[pl.BlockSpec(memory_space=pltpu.HBM)] * 5,
        out_specs=pl.BlockSpec(memory_space=pltpu.VMEM),
        scratch_shapes=[
            vm((width // block, rows, block), BF16),
            vm((groups + 1, width, block), BF16),
            vm((cols // block, w_out.shape[0], block), BF16),
            vm((heads, rows, VALUE_DIM), BF16),
            vm((rows, 128), BF16),
            vm((rows // chunk, 128, chunk), F32),
            vm((rows // chunk, 128, chunk), F32),
            vm((heads, rows // chunk, ROWS, chunk), BF16),
            vm((heads, rows // chunk, ROWS, 2 * VALUE_DIM), F32),
            vm((heads, rows, 2 * VALUE_DIM), F32),
            vm((heads, rows, ROWS), BF16),
            vm((groups, PLANE, PIECE, VALUE_DIM), BF16),
            vm((groups, PLANE, PIECE, VALUE_DIM), BF16),
            vm((groups, PIECE, VALUE_DIM), BF16),
            vm((groups, planes, PIECE, VALUE_DIM), BF16),
            vm((groups, PLANE, PIECE, VALUE_DIM), BF16),
            vm((groups, PLANE, PIECE, VALUE_DIM), BF16),
            vm((cols // block, rows, block), F32),
            dma((groups + 1, 2)), dma((LOADS, width // block)), dma((cols // block,)),
            dma((groups, PLANE)), dma((groups, PLANE)),
            dma((groups, planes)), dma((groups, planes)),
            dma((groups, PLANE)), dma((groups, PLANE)),
            dma((groups,)), dma((groups,)), pltpu.SemaphoreType.REGULAR,
        ],
        compiler_params=pltpu.CompilerParams(
            collective_id=0, has_side_effects=True, vmem_limit_bytes=VMEM_LIMIT
        ),
    )(*(pltpu.with_memory_space_constraint(a, pltpu.HBM) for a in (tokens, w_query, w_key, w_value, w_out)))


def solution(mesh):
    in_specs = (P("seq", None), P(None, "head"), P(None, "head"), P(None, "head"), P())
    return jax.shard_map(
        per_device, mesh=mesh, in_specs=in_specs, out_specs=P("seq", "head"), check_vma=False
    )
```
